32 devices in a mesh: tile: 8 (over z, y), rep: 4 (over x, core).
Axes of the slice: x: 2, y: 2, z: 4, core: 2. Of those that a mesh axis runs over, the one named last changes fastest.
Arguments:
- amplitudes: bfloat16 [1024, 8192], P(None, ('tile', 'rep')), may hold values from -3 to 3
- integrals: bfloat16 [4, 512, 128, 128], P('rep', 'tile'), may hold values from -0.1875 to 0.1875
- slot_row: int32 [4, 512], P('rep', 'tile'), may hold values from 0 to 7, as said below
- slot_col: int32 [4, 512], P('rep', 'tile'), may hold values from 0 to 15
- slot_count: int32 [4, 8], P('rep', 'tile'), may hold values from 32 to 64, as said below
- source: float32 [1024, 8192], P(None, ('tile', 'rep')), may hold values from -6 to 6
- occ_energy: float32 [1024], replicated, may hold values from -2 to -0.4
- virt_energy: float32 [8192], P(('tile', 'rep')), may hold values from 0.5 to 6.5
Outputs:
- residual: float32 [1024, 8192], P(None, ('tile', 'rep'))
- updated: float32 [1024, 8192], P(None, ('tile', 'rep'))
The draws below stay inside these ranges and needn't reach their ends.
Inputs may be any that keep to these rules, and one draw needn't show every extreme that they name: `slot_row`: within one device's 64 slots no pair of row tile and contraction tile occurs twice. `slot_count`: some device has all 64 slots live.
All inputs are finite; a program needn't handle non-finite values.
Results may differ from the reference program's by a relative error of at most 0.0003.
Values may be sent and summed in bfloat16 or wider, within the bound.
A program may use at most 128 MiB of HBM per device.

```python
import jax
import jax.numpy as jnp
from jax import lax

BT = 128
OPAIRS = 1024
PT_DEV = 8
P_SIZE = 64
QR = 16
NLOC = 64
N_TILE = 8
N_REP = 4


def slot_layout(key):
    keys = jax.random.split(jax.random.fold_in(key, 5), N_REP * N_TILE)

    def one_device(sub):
        return jax.random.permutation(sub, PT_DEV * QR)[:NLOC]
    picks = jax.vmap(one_device)(keys)
    return picks.reshape(N_REP, N_TILE * NLOC).astype(jnp.int32)


def draw_slot_row(key, part):
    return (slot_layout(key) // QR).astype(jnp.int32)


def draw_slot_col(key, part):
    return (slot_layout(key) % QR).astype(jnp.int32)


def draw_slot_count(key, part):
    keys = jax.random.split(jax.random.fold_in(key, 11), 2)
    counts = jax.random.randint(keys[0], (N_REP * N_TILE,), NLOC // 2, NLOC + 1)
    busiest = jax.random.randint(keys[1], (), 0, N_REP * N_TILE)
    counts = jnp.where(jnp.arange(N_REP * N_TILE) == busiest, NLOC, counts)
    return counts.reshape(N_REP, N_TILE).astype(jnp.int32)


def draw_virt_energy(key, part):
    raw = jax.random.uniform(key, (P_SIZE * BT,), jnp.float32, 0.2, 1.0)
    level = jnp.cumsum(raw)
    return (0.5 + 6.0 * level / level[-1]).astype(jnp.float32)


def block_scale(stream_key, dims, shards, least, largest):
    def one(axis_at, shards_of):
        draws = jax.random.uniform(jax.random.fold_in(jax.random.fold_in(stream_key, 6), axis_at), (shards_of,), jnp.float32, least / len(shards), largest / len(shards))
        return jnp.repeat(jnp.exp(draws), dims[axis_at] // shards_of).reshape((-1,) + (1,) * (len(dims) - axis_at - 1))

    factor_of = one(*shards[0])
    for cut in shards[1:]:
        factor_of = factor_of * one(*cut)
    return factor_of


def noise(own_key, extent, width, reach, shards=(), kind=jnp.bfloat16):
    level = block_scale(own_key, extent, shards, -0.22, 0.18) if shards else 1.0
    values = jax.random.normal(own_key, extent, jnp.float32) * width * level
    return jnp.minimum(jnp.maximum(values, -reach), reach).astype(kind)


def setup_inputs(seed: int = 0) -> dict:
    splits = jax.random.split(jax.random.key(seed), 9)
    amplitudes = noise(splits[0], (OPAIRS, P_SIZE * BT), 0.5, 3.0, ((1, 32),))
    integrals = noise(splits[1], (N_REP, N_TILE * NLOC, BT, BT), (NLOC * BT // 8) ** -0.5, 0.1875, ((0, 4), (1, 8)))
    slot_row = draw_slot_row(jax.random.fold_in(splits[8], 71), 0)
    slot_col = draw_slot_col(jax.random.fold_in(splits[8], 71), 0)
    slot_count = draw_slot_count(jax.random.fold_in(splits[8], 71), 0)
    source = noise(splits[5], (OPAIRS, P_SIZE * BT), 1.0, 6.0, ((1, 32),), jnp.float32)
    occ_energy = jnp.clip(jax.random.uniform(splits[6], (OPAIRS,), jnp.float32, -2.0, -0.4), -2.0, -0.4)
    virt_energy = draw_virt_energy(jax.random.fold_in(splits[8], 71), 0)
    return dict(amplitudes=amplitudes, integrals=integrals, slot_row=slot_row, slot_col=slot_col, slot_count=slot_count, source=source, occ_energy=occ_energy, virt_energy=virt_energy)


slot_block = 16
trust = 0.1

def slot_terms(tiles, ints, rows, cols, count):
    opairs = tiles.shape[0]
    edge = tiles.shape[2]

    def add_block(index, total):
        start = (index * slot_block).astype(jnp.int32)
        vblock = lax.dynamic_slice_in_dim(ints, start, slot_block, 0).astype(jnp.float32)
        rblock = lax.dynamic_slice_in_dim(rows, start, slot_block, 0)
        cblock = lax.dynamic_slice_in_dim(cols, start, slot_block, 0)
        picked = jnp.take(tiles, cblock, axis=1)
        terms = jnp.einsum('osc,sec->soe', picked, vblock, precision=lax.Precision.HIGHEST)
        where = start + lax.iota(jnp.int32, slot_block)
        live = where < count
        select = ((rblock[:, None] == lax.iota(jnp.int32, PT_DEV)[None, :]) & live[:, None]).astype(terms.dtype)
        return total + jnp.einsum('sk,soe->oke', select, terms, precision=lax.Precision.HIGHEST)
    total = jnp.zeros((opairs, PT_DEV, edge), jnp.float32)
    upper = ((count + slot_block - 1) // slot_block).astype(jnp.int32)
    total = lax.fori_loop(jnp.int32(0), upper, add_block, total)
    return total.reshape(opairs, PT_DEV * edge)

def reference(amplitudes, integrals, slot_row, slot_col, slot_count, source, occ_energy, virt_energy):
    opairs = amplitudes.shape[0]
    quarter = PT_DEV // N_REP
    blocks = amplitudes.reshape(opairs, N_TILE, N_REP, quarter * BT)
    ladder = jnp.zeros((N_TILE, opairs, PT_DEV * BT), jnp.float32)
    for group in range(N_REP):
        tiles = blocks[:, :, group, :].reshape(opairs, N_TILE * quarter, BT).astype(jnp.float32)
        ints = integrals[group].reshape(N_TILE, NLOC, BT, BT)
        rows = slot_row[group].reshape(N_TILE, NLOC)
        cols = slot_col[group].reshape(N_TILE, NLOC)

        def one_device(packed):
            return slot_terms(tiles, packed[0], packed[1], packed[2], packed[3])
        ladder = ladder + lax.map(one_device, (ints, rows, cols, slot_count[group]))
    ladder = jnp.transpose(ladder, (1, 0, 2)).reshape(opairs, P_SIZE * BT)
    residual = source + ladder
    step = residual / (virt_energy[None, :] - occ_energy[:, None])
    scale = jnp.minimum(1.0, trust / jnp.sqrt(jnp.mean(step * step) + 1e-06))
    updated = amplitudes.astype(jnp.float32) + scale * step
    return (residual, updated)
```

```python
import functools

import jax
import jax.numpy as jnp
from jax import lax
from jax.experimental import pallas as pl
from jax.experimental.pallas import tpu as pltpu
from jax.sharding import PartitionSpec as P

BT = 128
PT_DEV = 8
trust = 0.1
CHUNKS = 16
AHEAD = 4
MESH = pl.DeviceIdType.MESH


def cross_chunk(j):
    return lax.rem(j, 5) == 2


def kernel(
    nt, nr, nc,
    amp, ints, row, col, cnt, src, occ, virt,
    res_out, upd_out,
    gat, tiles, dense, inv_v, inv_s, occ_col, give, keep, core_in, x_out, x_in, src_v, res_v, step_v,
    sq, stat_a, stat_b, mine,
    su, sd, sy, rg, ds_, dr, xs, xr, sas, sar, sbs, sbr, loc, rsem, usem,
):
    t = lax.axis_index("tile")
    r = lax.axis_index("rep")
    rows_all, cols = amp.shape
    rc = rows_all // nc
    nloc = ints.shape[1]
    line = nt // 2
    q = cols // BT
    qr = nt * q
    nh = nr // 2
    l = t // 2
    y = lax.rem(t, 2)
    h = r // 2
    c = lax.rem(r, 2)

    amp_in = pltpu.make_async_copy(amp, gat.at[t], loc.at[0])
    amp_in.start()
    ints_in = pltpu.make_async_copy(ints.at[0], tiles.at[pl.ds(0, nloc)], loc.at[1])
    ints_in.start()
    src_in = pltpu.make_async_copy(src, src_v, loc.at[2])
    src_in.start()

    barrier = pltpu.get_barrier_semaphore()
    for k in range(1, nt):
        pl.semaphore_signal(barrier, inc=1, device_id={"tile": lax.rem(t + k, nt)}, device_id_type=MESH)
    for k in range(1, nr):
        pl.semaphore_signal(barrier, inc=1, device_id={"rep": lax.rem(r + k, nr)}, device_id_type=MESH)
    pl.semaphore_wait(barrier, nt - 1 + nr - 1)

    def piece(source, j, sem, dest):
        ref = gat.at[source, pl.ds(pl.multiple_of(j * rc, rc), rc)]
        return pltpu.make_async_remote_copy(
            src_ref=ref, dst_ref=ref, send_sem=sem.at[source, j], recv_sem=rg.at[source, j],
            device_id={"tile": dest}, device_id_type=MESH,
        )

    up_to = lax.rem(t + 2, nt)
    down_to = lax.rem(t + nt - 2, nt)
    across = t + 1 - 2 * y

    def up(source, j):
        return piece(source, j, su, up_to)

    def down(source, j):
        return piece(source, j, sd, down_to)

    def side(source, j):
        return piece(source, j, sy, across)

    def send_own(j):
        side(t, j).start()

        @pl.when(l < line - 1)
        def _():
            up(t, j).start()

        @pl.when(l > 0)
        def _():
            down(t, j).start()

    amp_in.wait()
    for j in range(AHEAD):
        send_own(j)

    key = row[...] * qr + col[...]
    where = lax.broadcasted_iota(jnp.int32, (1, nloc), 1)
    key = jnp.where(where < cnt[...], key, -1)
    diag = lax.broadcasted_iota(jnp.int32, (nloc, nloc), 0) == lax.broadcasted_iota(jnp.int32, (nloc, nloc), 1)
    key_col = jnp.sum(jnp.where(diag, jnp.broadcast_to(key, (nloc, nloc)), 0), axis=1, keepdims=True)
    pairs = PT_DEV * qr
    hit = key_col == lax.broadcasted_iota(jnp.int32, (nloc, pairs), 1)
    slot = lax.broadcasted_iota(jnp.int32, (nloc, pairs), 0)
    found = nloc - jnp.sum(jnp.where(hit, nloc - slot, 0), axis=0, keepdims=True)
    inv_v[...] = jnp.broadcast_to(found, inv_v.shape)
    inv_in = pltpu.make_async_copy(inv_v, inv_s, loc.at[3])
    inv_in.start()

    sq[...] = jnp.zeros_like(sq)
    tiles[nloc] = jnp.zeros((BT, BT), tiles.dtype)
    eye = lax.broadcasted_iota(jnp.int32, (BT, BT), 0) == lax.broadcasted_iota(jnp.int32, (BT, BT), 1)
    for k in range(rows_all // BT):
        part = jnp.broadcast_to(occ[:, k * BT : (k + 1) * BT], (BT, BT))
        occ_col[k * BT : (k + 1) * BT, :] = jnp.sum(jnp.where(eye, part, 0.0), axis=1, keepdims=True)
    inv_in.wait()
    ints_in.wait()

    def build(b, carry):
        for k in range(PT_DEV):
            for m in range(q):
                at = inv_s[0, k * qr + b * q + m]
                dense[k * BT : (k + 1) * BT, pl.ds(pl.multiple_of(b * cols + m * BT, BT), BT)] = tiles[at]
        return carry

    lax.fori_loop(0, nt, build, 0)
    src_in.wait()

    def core_copy(j):
        return pltpu.make_async_remote_copy(
            src_ref=give.at[j], dst_ref=core_in.at[j], send_sem=ds_.at[j], recv_sem=dr.at[j],
            device_id={"rep": r + 1 - 2 * c}, device_id_type=MESH,
        )

    def x_copy(j, m):
        return pltpu.make_async_remote_copy(
            src_ref=x_out.at[j, m - 1], dst_ref=x_in.at[j, m - 1], send_sem=xs.at[j, m - 1], recv_sem=xr.at[j, m - 1],
            device_id={"rep": lax.rem(h + m, nh) * 2 + c}, device_id_type=MESH,
        )

    def res_copy(j):
        span = pl.ds(pl.multiple_of(j * rc, rc), rc)
        return pltpu.make_async_copy(res_v.at[span], res_out.at[span], rsem.at[j])

    latest = line

    def inside(j):
        return (j >= 0) & (j < nc)

    def forward(d, i):
        j = i - d + 1

        @pl.when(inside(j) & (d > 0))
        def _():
            @pl.when(l - d >= 0)
            def _():
                source = t - 2 * d
                up(source, j).wait_recv()

                @pl.when(l < line - 1)
                def _():
                    up(source, j).start()

                @pl.when(jnp.logical_not(cross_chunk(j)))
                def _():
                    side(source, j).start()

            @pl.when(l + d < line)
            def _():
                source = t + 2 * d
                down(source, j).wait_recv()

                @pl.when(l > 0)
                def _():
                    down(source, j).start()

                @pl.when(jnp.logical_not(cross_chunk(j)))
                def _():
                    side(source, j).start()

        m = i - d

        @pl.when(inside(m) & cross_chunk(m))
        def _():
            @pl.when(d == 0)
            def _():
                side(across, m).wait_recv()

                @pl.when(l < line - 1)
                def _():
                    up(across, m).start()

                @pl.when(l > 0)
                def _():
                    down(across, m).start()

            @pl.when((d > 0) & (l - d >= 0))
            def _():
                source = across - 2 * d
                up(source, m).wait_recv()

                @pl.when(l < line - 1)
                def _():
                    up(source, m).start()

            @pl.when((d > 0) & (l + d < line))
            def _():
                source = across + 2 * d
                down(source, m).wait_recv()

                @pl.when(l > 0)
                def _():
                    down(source, m).start()

        return i

    def drain(b, j):
        source = 2 * b + y
        other = 2 * b + 1 - y

        @pl.when((l < line - 1) & (b <= l))
        def _():
            up(source, j).wait_send()

            @pl.when(cross_chunk(j))
            def _():
                up(other, j).wait_send()

        @pl.when((l > 0) & (b >= l))
        def _():
            down(source, j).wait_send()

            @pl.when(cross_chunk(j))
            def _():
                down(other, j).wait_send()

        @pl.when((b == l) | jnp.logical_not(cross_chunk(j)))
        def _():
            side(source, j).wait_send()

        return j

    def multiply(lhs, block):
        w = dense[pl.ds(pl.multiple_of(block * cols, cols), cols), :]
        return lax.dot_general(lhs, w, (((1,), (1,)), ((), ())), preferred_element_type=jnp.float32)

    def main(i, carry):
        @pl.when(i + AHEAD < nc)
        def _():
            send_own(i + AHEAD)

        lax.fori_loop(0, line, forward, i)

        j = i - latest

        @pl.when(inside(j))
        def _():
            @pl.when(jnp.logical_not(cross_chunk(j)))
            def _():
                def arrived(b, carry):
                    side(2 * b + 1 - y, j).wait_recv()
                    return carry

                lax.fori_loop(0, line, arrived, 0)

            span = pl.ds(pl.multiple_of(j * rc, rc), rc)
            lhs = jnp.concatenate([gat[b, span, :] for b in range(nt)], axis=1)
            for m in range(nh):
                give[j, m] = multiply(lhs, 2 * m + 1 - c)
            core_copy(j).start()
            for m in range(nh):
                keep[j, m] = multiply(lhs, 2 * lax.rem(h + m, nh) + c)

        k = j - 1

        @pl.when(inside(k))
        def _():
            core_copy(k).wait_recv()
            for m in range(1, nh):
                x_out[k, m - 1] = keep[k, m] + core_in[k, lax.rem(h + m, nh)]
                x_copy(k, m).start()

        n = j - 2

        @pl.when(inside(n))
        def _():
            total = keep[n, 0] + core_in[n, h]
            for m in range(1, nh):
                x_copy(n, m).wait_recv()
                total = total + x_in[n, m - 1]
            span = pl.ds(pl.multiple_of(n * rc, rc), rc)
            residual = src_v[span, :] + total
            res_v[span, :] = residual
            step = residual / (virt[...] - occ_col[span, :])
            step_v[span, :] = step
            square = jnp.sum((step * step).reshape(rc // 8, 8, cols), axis=0)
            part = square[:, :BT]
            for m in range(1, q):
                part = part + square[:, m * BT : (m + 1) * BT]
            sq[...] += part
            res_copy(n).start()

            @pl.when(n < nc - 1)
            def _():
                lax.fori_loop(0, line, drain, n)
                core_copy(n).wait_send()
                for m in range(1, nh):
                    x_copy(n, m).wait_send()

        return carry

    lax.fori_loop(0, nc + latest + 2, main, 0)

    def stat_rep(m):
        return pltpu.make_async_remote_copy(
            src_ref=sq, dst_ref=stat_a.at[m - 1], send_sem=sas.at[m - 1], recv_sem=sar.at[m - 1],
            device_id={"rep": lax.rem(r + m, nr)}, device_id_type=MESH,
        )

    def stat_tile(m):
        return pltpu.make_async_remote_copy(
            src_ref=mine, dst_ref=stat_b.at[m - 1], send_sem=sbs.at[m - 1], recv_sem=sbr.at[m - 1],
            device_id={"tile": lax.rem(t + m, nt)}, device_id_type=MESH,
        )

    for m in range(1, nr):
        stat_rep(m).start()
    total = sq[...]
    for m in range(1, nr):
        stat_rep(m).wait_recv()
        total = total + stat_a[m - 1]
    mine[...] = total
    for m in range(1, nt):
        stat_tile(m).start()
    for m in range(1, nt):
        stat_tile(m).wait_recv()
        total = total + stat_b[m - 1]
    mean = jnp.sum(total, keepdims=True) / (rows_all * cols * nt * nr)
    scale = jnp.minimum(1.0, trust / jnp.sqrt(mean + 1e-06))

    def finish(j, carry):
        span = pl.ds(pl.multiple_of(j * rc, rc), rc)
        step_v[span, :] = gat[t, span, :].astype(jnp.float32) + scale * step_v[span, :]
        pltpu.make_async_copy(step_v.at[span], upd_out.at[span], usem.at[j]).start()
        return carry

    lax.fori_loop(0, nc, finish, 0)

    lax.fori_loop(0, line, drain, nc - 1)
    core_copy(nc - 1).wait_send()
    for m in range(1, nh):
        x_copy(nc - 1, m).wait_send()
    for m in range(1, nr):
        stat_rep(m).wait_send()
    for m in range(1, nt):
        stat_tile(m).wait_send()

    def written(j, carry):
        span = pl.ds(pl.multiple_of(j * rc, rc), rc)
        res_copy(j).wait()
        pltpu.make_async_copy(step_v.at[span], upd_out.at[span], usem.at[j]).wait()
        return carry

    lax.fori_loop(0, nc, written, 0)


def local(nt, nr, amplitudes, integrals, slot_row, slot_col, slot_count, source, occ_energy, virt_energy):
    rows, cols = amplitudes.shape
    nloc = integrals.shape[1]
    nc = CHUNKS
    rc = rows // nc
    nh = nr // 2
    qr = nt * (cols // BT)
    pairs = PT_DEV * qr
    f32 = jnp.float32
    dma = pltpu.SemaphoreType.DMA
    vmem = pl.BlockSpec(memory_space=pltpu.VMEM)
    anywhere = pl.BlockSpec(memory_space=pl.ANY)
    scratch = [
        pltpu.VMEM((nt, rows, cols), jnp.bfloat16),
        pltpu.VMEM((nloc + 1, BT, BT), jnp.bfloat16),
        pltpu.VMEM((PT_DEV * BT, nt * cols), jnp.bfloat16),
        pltpu.VMEM((8, pairs), jnp.int32),
        pltpu.SMEM((8, pairs), jnp.int32),
        pltpu.VMEM((rows, 1), f32),
        pltpu.VMEM((nc, nh, rc, cols), f32),
        pltpu.VMEM((nc, nh, rc, cols), f32),
        pltpu.VMEM((nc, nh, rc, cols), f32),
        pltpu.VMEM((nc, nh - 1, rc, cols), f32),
        pltpu.VMEM((nc, nh - 1, rc, cols), f32),
        pltpu.VMEM((rows, cols), f32),
        pltpu.VMEM((rows, cols), f32),
        pltpu.VMEM((rows, cols), f32),
        pltpu.VMEM((8, BT), f32),
        pltpu.VMEM((nr - 1, 8, BT), f32),
        pltpu.VMEM((nt - 1, 8, BT), f32),
        pltpu.VMEM((8, BT), f32),
        dma((nt, nc)), dma((nt, nc)), dma((nt, nc)), dma((nt, nc)),
        dma((nc,)), dma((nc,)), dma((nc, nh - 1)), dma((nc, nh - 1)),
        dma((nr - 1,)), dma((nr - 1,)), dma((nt - 1,)), dma((nt - 1,)),
        dma((4,)), dma((nc,)), dma((nc,)),
    ]
    out = jax.ShapeDtypeStruct((rows, cols), f32)
    return pl.pallas_call(
        functools.partial(kernel, nt, nr, nc),
        out_shape=(out, out),
        in_specs=[anywhere, anywhere, vmem, vmem, vmem, anywhere, vmem, vmem],
        out_specs=(anywhere, anywhere),
        scratch_shapes=scratch,
        compiler_params=pltpu.CompilerParams(
            collective_id=0, has_side_effects=True, vmem_limit_bytes=61 * 1024 * 1024
        ),
        name="ladder",
    )(
        amplitudes, integrals, slot_row, slot_col, slot_count, source,
        occ_energy.reshape(1, rows), virt_energy.reshape(1, cols),
    )


def solution(mesh):
    placed = (
        P(None, ("tile", "rep")),
        P("rep", "tile", None, None),
        P("rep", "tile"),
        P("rep", "tile"),
        P("rep", "tile"),
        P(None, ("tile", "rep")),
        P(),
        P(("tile", "rep")),
    )
    return jax.shard_map(
        functools.partial(local, mesh.shape["tile"], mesh.shape["rep"]),
        mesh=mesh,
        in_specs=placed,
        out_specs=(P(None, ("tile", "rep")), P(None, ("tile", "rep"))),
        check_vma=False,
    )
```

```python
import functools

import jax
import jax.numpy as jnp
from jax import lax
from jax.experimental import pallas as pl
from jax.experimental.pallas import tpu as pltpu
from jax.sharding import PartitionSpec as P

BT = 128
PT_DEV = 8
trust = 0.1
CHUNKS = 8
AHEAD = 4
MESH = pl.DeviceIdType.MESH


def cross_chunk(j):
    return lax.rem(j, 8) == 3


def kernel(
    nt, nr, nc,
    amp, ints, row, col, cnt, src, occ, virt,
    lad_out, scale_out,
    gat, tiles, dense, inv_v, inv_s, occ_col, give, keep, core_in, x_out, x_in, src_v, lad_v,
    sq, stat_a, stat_b, mine,
    su, sd, sy, rg, ds_, dr, xs, xr, sas, sar, sbs, sbr, loc, rsem,
):
    t = lax.axis_index("tile")
    r = lax.axis_index("rep")
    rows_all, cols = amp.shape
    rc = rows_all // nc
    nloc = ints.shape[1]
    line = nt // 2
    q = cols // BT
    qr = nt * q
    nh = nr // 2
    l = t // 2
    y = lax.rem(t, 2)
    h = r // 2
    c = lax.rem(r, 2)

    amp_in = pltpu.make_async_copy(amp, gat.at[t], loc.at[0])
    amp_in.start()
    ints_in = pltpu.make_async_copy(ints.at[0], tiles.at[pl.ds(0, nloc)], loc.at[1])
    ints_in.start()
    src_in = pltpu.make_async_copy(src, src_v, loc.at[2])
    src_in.start()

    barrier = pltpu.get_barrier_semaphore()
    for k in range(1, nt):
        pl.semaphore_signal(barrier, inc=1, device_id={"tile": lax.rem(t + k, nt)}, device_id_type=MESH)
    for k in range(1, nr):
        pl.semaphore_signal(barrier, inc=1, device_id={"rep": lax.rem(r + k, nr)}, device_id_type=MESH)
    pl.semaphore_wait(barrier, nt - 1 + nr - 1)

    def piece(source, j, sem, dest):
        ref = gat.at[source, pl.ds(pl.multiple_of(j * rc, rc), rc)]
        return pltpu.make_async_remote_copy(
            src_ref=ref, dst_ref=ref, send_sem=sem.at[source, j], recv_sem=rg.at[source, j],
            device_id={"tile": dest}, device_id_type=MESH,
        )

    up_to = lax.rem(t + 2, nt)
    down_to = lax.rem(t + nt - 2, nt)
    across = t + 1 - 2 * y

    def up(source, j):
        return piece(source, j, su, up_to)

    def down(source, j):
        return piece(source, j, sd, down_to)

    def side(source, j):
        return piece(source, j, sy, across)

    def send_own(j):
        side(t, j).start()

        @pl.when(l < line - 1)
        def _():
            up(t, j).start()

        @pl.when(l > 0)
        def _():
            down(t, j).start()

    amp_in.wait()
    for j in range(AHEAD):
        send_own(j)

    key = row[...] * qr + col[...]
    where = lax.broadcasted_iota(jnp.int32, (1, nloc), 1)
    key = jnp.where(where < cnt[...], key, -1)
    diag = lax.broadcasted_iota(jnp.int32, (nloc, nloc), 0) == lax.broadcasted_iota(jnp.int32, (nloc, nloc), 1)
    key_col = jnp.sum(jnp.where(diag, jnp.broadcast_to(key, (nloc, nloc)), 0), axis=1, keepdims=True)
    pairs = PT_DEV * qr
    hit = key_col == lax.broadcasted_iota(jnp.int32, (nloc, pairs), 1)
    slot = lax.broadcasted_iota(jnp.int32, (nloc, pairs), 0)
    found = nloc - jnp.sum(jnp.where(hit, nloc - slot, 0), axis=0, keepdims=True)
    inv_v[...] = jnp.broadcast_to(found, inv_v.shape)
    inv_in = pltpu.make_async_copy(inv_v, inv_s, loc.at[3])
    inv_in.start()

    sq[...] = jnp.zeros_like(sq)
    tiles[nloc] = jnp.zeros((BT, BT), tiles.dtype)
    eye = lax.broadcasted_iota(jnp.int32, (BT, BT), 0) == lax.broadcasted_iota(jnp.int32, (BT, BT), 1)
    for k in range(rows_all // BT):
        part = jnp.broadcast_to(occ[:, k * BT : (k + 1) * BT], (BT, BT))
        occ_col[k * BT : (k + 1) * BT, :] = jnp.sum(jnp.where(eye, part, 0.0), axis=1, keepdims=True)
    inv_in.wait()
    ints_in.wait()

    def build(b, carry):
        for k in range(PT_DEV):
            for m in range(q):
                at = inv_s[0, k * qr + b * q + m]
                dense[k * BT : (k + 1) * BT, pl.ds(pl.multiple_of(b * cols + m * BT, BT), BT)] = tiles[at]
        return carry

    lax.fori_loop(0, nt, build, 0)
    src_in.wait()

    def core_copy(j, m):
        return pltpu.make_async_remote_copy(
            src_ref=give.at[j, m], dst_ref=core_in.at[j, m], send_sem=ds_.at[j, m], recv_sem=dr.at[j, m],
            device_id={"rep": r + 1 - 2 * c}, device_id_type=MESH,
        )

    def x_copy(j, m):
        return pltpu.make_async_remote_copy(
            src_ref=x_out.at[j, m - 1], dst_ref=x_in.at[j, m - 1], send_sem=xs.at[j, m - 1], recv_sem=xr.at[j, m - 1],
            device_id={"rep": lax.rem(h + m, nh) * 2 + c}, device_id_type=MESH,
        )

    def lad_copy(j):
        span = pl.ds(pl.multiple_of(j * rc, rc), rc)
        return pltpu.make_async_copy(lad_v.at[span], lad_out.at[span], rsem.at[j])

    latest = line

    def inside(j):
        return (j >= 0) & (j < nc)

    def forward(d, i):
        j = i - d + 1

        @pl.when(inside(j) & (d > 0))
        def _():
            @pl.when(l - d >= 0)
            def _():
                source = t - 2 * d
                up(source, j).wait_recv()

                @pl.when(l < line - 1)
                def _():
                    up(source, j).start()

                @pl.when(jnp.logical_not(cross_chunk(j)))
                def _():
                    side(source, j).start()

            @pl.when(l + d < line)
            def _():
                source = t + 2 * d
                down(source, j).wait_recv()

                @pl.when(l > 0)
                def _():
                    down(source, j).start()

                @pl.when(jnp.logical_not(cross_chunk(j)))
                def _():
                    side(source, j).start()

        m = i - d

        @pl.when(inside(m) & cross_chunk(m))
        def _():
            @pl.when(d == 0)
            def _():
                side(across, m).wait_recv()

                @pl.when(l < line - 1)
                def _():
                    up(across, m).start()

                @pl.when(l > 0)
                def _():
                    down(across, m).start()

            @pl.when((d > 0) & (l - d >= 0))
            def _():
                source = across - 2 * d
                up(source, m).wait_recv()

                @pl.when(l < line - 1)
                def _():
                    up(source, m).start()

            @pl.when((d > 0) & (l + d < line))
            def _():
                source = across + 2 * d
                down(source, m).wait_recv()

                @pl.when(l > 0)
                def _():
                    down(source, m).start()

        return i

    def drain(b, j):
        source = 2 * b + y
        other = 2 * b + 1 - y

        @pl.when((l < line - 1) & (b <= l))
        def _():
            up(source, j).wait_send()

            @pl.when(cross_chunk(j))
            def _():
                up(other, j).wait_send()

        @pl.when((l > 0) & (b >= l))
        def _():
            down(source, j).wait_send()

            @pl.when(cross_chunk(j))
            def _():
                down(other, j).wait_send()

        @pl.when((b == l) | jnp.logical_not(cross_chunk(j)))
        def _():
            side(source, j).wait_send()

        return j

    def multiply(lhs, block):
        w = dense[pl.ds(pl.multiple_of(block * cols, cols), cols), :]
        return lax.dot_general(lhs, w, (((1,), (1,)), ((), ())), preferred_element_type=jnp.float32)

    def main(i, carry):
        @pl.when(i + AHEAD < nc)
        def _():
            send_own(i + AHEAD)

        lax.fori_loop(0, line, forward, i)

        j = i - latest

        @pl.when(inside(j))
        def _():
            @pl.when(jnp.logical_not(cross_chunk(j)))
            def _():
                def arrived(b, carry):
                    side(2 * b + 1 - y, j).wait_recv()
                    return carry

                lax.fori_loop(0, line, arrived, 0)

            span = pl.ds(pl.multiple_of(j * rc, rc), rc)
            lhs = jnp.concatenate([gat[b, span, :] for b in range(nt)], axis=1)
            order = list(range(1, nh)) + [0]
            for m in order:
                give[j, m] = multiply(lhs, 2 * lax.rem(h + m, nh) + 1 - c)
                core_copy(j, m).start()
            for m in order:
                keep[j, m] = multiply(lhs, 2 * lax.rem(h + m, nh) + c)
            for m in range(1, nh):
                core_copy(j, m).wait_recv()
                x_out[j, m - 1] = keep[j, m] + core_in[j, m]
                x_copy(j, m).start()

        n = j - 1

        @pl.when(inside(n))
        def _():
            core_copy(n, 0).wait_recv()
            total = keep[n, 0] + core_in[n, 0]
            for m in range(1, nh):
                x_copy(n, m).wait_recv()
                total = total + x_in[n, m - 1]
            span = pl.ds(pl.multiple_of(n * rc, rc), rc)
            residual = src_v[span, :] + total
            lad_v[span, :] = total
            lad_copy(n).start()
            step = residual / (virt[...] - occ_col[span, :])
            square = jnp.sum((step * step).reshape(rc // 8, 8, cols), axis=0)
            part = square[:, :BT]
            for m in range(1, q):
                part = part + square[:, m * BT : (m + 1) * BT]
            sq[...] += part

            @pl.when(n < nc - 1)
            def _():
                lax.fori_loop(0, line, drain, n)
                for m in range(nh):
                    core_copy(n, m).wait_send()
                for m in range(1, nh):
                    x_copy(n, m).wait_send()

        return carry

    lax.fori_loop(0, nc + latest + 1, main, 0)

    def stat_rep(m):
        return pltpu.make_async_remote_copy(
            src_ref=sq, dst_ref=stat_a.at[m - 1], send_sem=sas.at[m - 1], recv_sem=sar.at[m - 1],
            device_id={"rep": lax.rem(r + m, nr)}, device_id_type=MESH,
        )

    def stat_tile(m):
        return pltpu.make_async_remote_copy(
            src_ref=mine, dst_ref=stat_b.at[m - 1], send_sem=sbs.at[m - 1], recv_sem=sbr.at[m - 1],
            device_id={"tile": lax.rem(t + m, nt)}, device_id_type=MESH,
        )

    for m in range(1, nr):
        stat_rep(m).start()
    total = sq[...]

    lax.fori_loop(0, line, drain, nc - 1)
    for m in range(nh):
        core_copy(nc - 1, m).wait_send()
    for m in range(1, nh):
        x_copy(nc - 1, m).wait_send()

    for m in range(1, nr):
        stat_rep(m).wait_recv()
        total = total + stat_a[m - 1]
    mine[...] = total
    for m in range(1, nt):
        stat_tile(m).start()

    def written(j, carry):
        lad_copy(j).wait()
        return carry

    lax.fori_loop(0, nc, written, 0)
    for m in range(1, nr):
        stat_rep(m).wait_send()
    for m in range(1, nt):
        stat_tile(m).wait_recv()
        total = total + stat_b[m - 1]
    mean = jnp.sum(total, keepdims=True) / (rows_all * cols * nt * nr)
    scale = jnp.minimum(1.0, trust / jnp.sqrt(mean + 1e-06))
    scale_out[...] = jnp.broadcast_to(scale, scale_out.shape)
    for m in range(1, nt):
        stat_tile(m).wait_send()


def local(nt, nr, amplitudes, integrals, slot_row, slot_col, slot_count, source, occ_energy, virt_energy):
    rows, cols = amplitudes.shape
    nloc = integrals.shape[1]
    nc = CHUNKS
    rc = rows // nc
    nh = nr // 2
    qr = nt * (cols // BT)
    pairs = PT_DEV * qr
    f32 = jnp.float32
    dma = pltpu.SemaphoreType.DMA
    vmem = pl.BlockSpec(memory_space=pltpu.VMEM)
    anywhere = pl.BlockSpec(memory_space=pl.ANY)
    scratch = [
        pltpu.VMEM((nt, rows, cols), jnp.bfloat16),
        pltpu.VMEM((nloc + 1, BT, BT), jnp.bfloat16),
        pltpu.VMEM((PT_DEV * BT, nt * cols), jnp.bfloat16),
        pltpu.VMEM((8, pairs), jnp.int32),
        pltpu.SMEM((8, pairs), jnp.int32),
        pltpu.VMEM((rows, 1), f32),
        pltpu.VMEM((nc, nh, rc, cols), f32),
        pltpu.VMEM((nc, nh, rc, cols), f32),
        pltpu.VMEM((nc, nh, rc, cols), f32),
        pltpu.VMEM((nc, nh - 1, rc, cols), f32),
        pltpu.VMEM((nc, nh - 1, rc, cols), f32),
        pltpu.VMEM((rows, cols), f32),
        pltpu.VMEM((rows, cols), f32),
        pltpu.VMEM((8, BT), f32),
        pltpu.VMEM((nr - 1, 8, BT), f32),
        pltpu.VMEM((nt - 1, 8, BT), f32),
        pltpu.VMEM((8, BT), f32),
        dma((nt, nc)), dma((nt, nc)), dma((nt, nc)), dma((nt, nc)),
        dma((nc, nh)), dma((nc, nh)), dma((nc, nh - 1)), dma((nc, nh - 1)),
        dma((nr - 1,)), dma((nr - 1,)), dma((nt - 1,)), dma((nt - 1,)),
        dma((4,)), dma((nc,)),
    ]
    ladder, scale = pl.pallas_call(
        functools.partial(kernel, nt, nr, nc),
        out_shape=(jax.ShapeDtypeStruct((rows, cols), f32), jax.ShapeDtypeStruct((1, cols), f32)),
        in_specs=[anywhere, anywhere, vmem, vmem, vmem, anywhere, vmem, vmem],
        out_specs=(anywhere, vmem),
        scratch_shapes=scratch,
        compiler_params=pltpu.CompilerParams(
            collective_id=0, has_side_effects=True, vmem_limit_bytes=60 * 1024 * 1024
        ),
        name="ladder",
    )(
        amplitudes, integrals, slot_row, slot_col, slot_count, source,
        occ_energy.reshape(1, rows), virt_energy.reshape(1, cols),
    )
    residual = source + ladder
    step = residual / (virt_energy[None, :] - occ_energy[:, None])
    return residual, amplitudes.astype(f32) + scale * step


def solution(mesh):
    placed = (
        P(None, ("tile", "rep")),
        P("rep", "tile", None, None),
        P("rep", "tile"),
        P("rep", "tile"),
        P("rep", "tile"),
        P(None, ("tile", "rep")),
        P(),
        P(("tile", "rep")),
    )
    return jax.shard_map(
        functools.partial(local, mesh.shape["tile"], mesh.shape["rep"]),
        mesh=mesh,
        in_specs=placed,
        out_specs=(P(None, ("tile", "rep")), P(None, ("tile", "rep"))),
        check_vma=False,
    )
```

```python
import functools

import jax
import jax.numpy as jnp
from jax import lax
from jax.experimental import pallas as pl
from jax.experimental.pallas import tpu as pltpu
from jax.sharding import PartitionSpec as P

BT = 128
PT_DEV = 8
trust = 0.1
CHUNKS = 8
AHEAD = 4
MESH = pl.DeviceIdType.MESH


def cross_chunk(j):
    return lax.rem(j, 8) == 7


def kernel(
    nt, nr, nc,
    amp, ints, row, col, cnt, src, occ, virt,
    lad_out, scale_out,
    gat, tiles, dense, inv_v, inv_s, occ_col, give, keep, core_in, x_out, x_in, src_v, lad_v,
    sq, stat_a, stat_b, mine,
    su, sd, sy, rg, ds_, dr, xs, xr, sas, sar, sbs, sbr, loc, rsem,
):
    t = lax.axis_index("tile")
    r = lax.axis_index("rep")
    rows_all, cols = amp.shape
    rc = rows_all // nc
    nloc = ints.shape[1]
    line = nt // 2
    q = cols // BT
    qr = nt * q
    nh = nr // 2
    l = t // 2
    y = lax.rem(t, 2)
    h = r // 2
    c = lax.rem(r, 2)

    amp_in = pltpu.make_async_copy(amp, gat.at[t], loc.at[0])
    amp_in.start()
    ints_in = pltpu.make_async_copy(ints.at[0], tiles.at[pl.ds(0, nloc)], loc.at[1])
    ints_in.start()
    src_in = pltpu.make_async_copy(src, src_v, loc.at[2])
    src_in.start()

    barrier = pltpu.get_barrier_semaphore()
    for k in range(1, nt):
        pl.semaphore_signal(barrier, inc=1, device_id={"tile": lax.rem(t + k, nt)}, device_id_type=MESH)
    for k in range(1, nr):
        pl.semaphore_signal(barrier, inc=1, device_id={"rep": lax.rem(r + k, nr)}, device_id_type=MESH)
    pl.semaphore_wait(barrier, nt - 1 + nr - 1)

    def piece(source, j, sem, dest):
        ref = gat.at[source, pl.ds(pl.multiple_of(j * rc, rc), rc)]
        return pltpu.make_async_remote_copy(
            src_ref=ref, dst_ref=ref, send_sem=sem.at[source, j], recv_sem=rg.at[source, j],
            device_id={"tile": dest}, device_id_type=MESH,
        )

    up_to = lax.rem(t + 2, nt)
    down_to = lax.rem(t + nt - 2, nt)
    across = t + 1 - 2 * y

    def up(source, j):
        return piece(source, j, su, up_to)

    def down(source, j):
        return piece(source, j, sd, down_to)

    def side(source, j):
        return piece(source, j, sy, across)

    def send_own(j):
        side(t, j).start()

        @pl.when(l < line - 1)
        def _():
            up(t, j).start()

        @pl.when(l > 0)
        def _():
            down(t, j).start()

    amp_in.wait()
    for j in range(AHEAD):
        send_own(j)

    key = row[...] * qr + col[...]
    where = lax.broadcasted_iota(jnp.int32, (1, nloc), 1)
    key = jnp.where(where < cnt[...], key, -1)
    diag = lax.broadcasted_iota(jnp.int32, (nloc, nloc), 0) == lax.broadcasted_iota(jnp.int32, (nloc, nloc), 1)
    key_col = jnp.sum(jnp.where(diag, jnp.broadcast_to(key, (nloc, nloc)), 0), axis=1, keepdims=True)
    pairs = PT_DEV * qr
    hit = key_col == lax.broadcasted_iota(jnp.int32, (nloc, pairs), 1)
    slot = lax.broadcasted_iota(jnp.int32, (nloc, pairs), 0)
    found = nloc - jnp.sum(jnp.where(hit, nloc - slot, 0), axis=0, keepdims=True)
    inv_v[...] = jnp.broadcast_to(found, inv_v.shape)
    inv_in = pltpu.make_async_copy(inv_v, inv_s, loc.at[3])
    inv_in.start()

    sq[...] = jnp.zeros_like(sq)
    tiles[nloc] = jnp.zeros((BT, BT), tiles.dtype)
    eye = lax.broadcasted_iota(jnp.int32, (BT, BT), 0) == lax.broadcasted_iota(jnp.int32, (BT, BT), 1)
    for k in range(rows_all // BT):
        part = jnp.broadcast_to(occ[:, k * BT : (k + 1) * BT], (BT, BT))
        occ_col[k * BT : (k + 1) * BT, :] = jnp.sum(jnp.where(eye, part, 0.0), axis=1, keepdims=True)
    inv_in.wait()
    ints_in.wait()

    def build(b, carry):
        for k in range(PT_DEV):
            for m in range(q):
                at = inv_s[0, k * qr + b * q + m]
                dense[k * BT : (k + 1) * BT, pl.ds(pl.multiple_of(b * cols + m * BT, BT), BT)] = tiles[at]
        return carry

    lax.fori_loop(0, nt, build, 0)
    src_in.wait()

    def core_copy(j, m):
        return pltpu.make_async_remote_copy(
            src_ref=give.at[j, m], dst_ref=core_in.at[j, m], send_sem=ds_.at[j, m], recv_sem=dr.at[j, m],
            device_id={"rep": r + 1 - 2 * c}, device_id_type=MESH,
        )

    def x_copy(j, m):
        return pltpu.make_async_remote_copy(
            src_ref=x_out.at[j, m - 1], dst_ref=x_in.at[j, m - 1], send_sem=xs.at[j, m - 1], recv_sem=xr.at[j, m - 1],
            device_id={"rep": lax.rem(h + m, nh) * 2 + c}, device_id_type=MESH,
        )

    def lad_copy(j):
        span = pl.ds(pl.multiple_of(j * rc, rc), rc)
        return pltpu.make_async_copy(lad_v.at[span], lad_out.at[span], rsem.at[j])

    latest = line - 1

    def inside(j):
        return (j >= 0) & (j < nc)

    def forward(d, i):
        j = i - d + 1

        @pl.when(inside(j) & (d > 0))
        def _():
            @pl.when(l - d >= 0)
            def _():
                source = t - 2 * d
                up(source, j).wait_recv()

                @pl.when(l < line - 1)
                def _():
                    up(source, j).start()

                @pl.when(jnp.logical_not(cross_chunk(j)))
                def _():
                    side(source, j).start()

            @pl.when(l + d < line)
            def _():
                source = t + 2 * d
                down(source, j).wait_recv()

                @pl.when(l > 0)
                def _():
                    down(source, j).start()

                @pl.when(jnp.logical_not(cross_chunk(j)))
                def _():
                    side(source, j).start()

        m = i - d

        @pl.when(inside(m) & cross_chunk(m))
        def _():
            @pl.when(d == 0)
            def _():
                side(across, m).wait_recv()

                @pl.when(l < line - 1)
                def _():
                    up(across, m).start()

                @pl.when(l > 0)
                def _():
                    down(across, m).start()

            @pl.when((d > 0) & (l - d >= 0))
            def _():
                source = across - 2 * d
                up(source, m).wait_recv()

                @pl.when(l < line - 1)
                def _():
                    up(source, m).start()

            @pl.when((d > 0) & (l + d < line))
            def _():
                source = across + 2 * d
                down(source, m).wait_recv()

                @pl.when(l > 0)
                def _():
                    down(source, m).start()

        return i

    def drain(b, j):
        source = 2 * b + y
        other = 2 * b + 1 - y

        @pl.when((l < line - 1) & (b <= l))
        def _():
            up(source, j).wait_send()

            @pl.when(cross_chunk(j))
            def _():
                up(other, j).wait_send()

        @pl.when((l > 0) & (b >= l))
        def _():
            down(source, j).wait_send()

            @pl.when(cross_chunk(j))
            def _():
                down(other, j).wait_send()

        @pl.when((b == l) | jnp.logical_not(cross_chunk(j)))
        def _():
            side(source, j).wait_send()

        return j

    def multiply(lhs, block):
        w = dense[pl.ds(pl.multiple_of(block * cols, cols), cols), :]
        return lax.dot_general(lhs, w, (((1,), (1,)), ((), ())), preferred_element_type=jnp.float32)

    def main(i, carry):
        @pl.when(i + AHEAD < nc)
        def _():
            send_own(i + AHEAD)

        lax.fori_loop(0, line, forward, i)

        j = i - latest

        @pl.when(inside(j))
        def _():
            @pl.when(jnp.logical_not(cross_chunk(j)))
            def _():
                def arrived(b, carry):
                    side(2 * b + 1 - y, j).wait_recv()
                    return carry

                lax.fori_loop(0, line, arrived, 0)

            span = pl.ds(pl.multiple_of(j * rc, rc), rc)
            lhs = jnp.concatenate([gat[b, span, :] for b in range(nt)], axis=1)
            order = list(range(1, nh)) + [0]
            for m in order:
                give[j, m] = multiply(lhs, 2 * lax.rem(h + m, nh) + 1 - c)
                core_copy(j, m).start()
            for m in order:
                keep[j, m] = multiply(lhs, 2 * lax.rem(h + m, nh) + c)
            for m in range(1, nh):
                core_copy(j, m).wait_recv()
                x_out[j, m - 1] = keep[j, m] + core_in[j, m]
                x_copy(j, m).start()

        n = j - 1

        @pl.when(inside(n))
        def _():
            core_copy(n, 0).wait_recv()
            total = keep[n, 0] + core_in[n, 0]
            for m in range(1, nh):
                x_copy(n, m).wait_recv()
                total = total + x_in[n, m - 1]
            span = pl.ds(pl.multiple_of(n * rc, rc), rc)
            residual = src_v[span, :] + total
            lad_v[span, :] = total
            lad_copy(n).start()
            step = residual / (virt[...] - occ_col[span, :])
            square = jnp.sum((step * step).reshape(rc // 8, 8, cols), axis=0)
            part = square[:, :BT]
            for m in range(1, q):
                part = part + square[:, m * BT : (m + 1) * BT]
            sq[...] += part

            @pl.when(n < nc - 1)
            def _():
                lax.fori_loop(0, line, drain, n)
                for m in range(nh):
                    core_copy(n, m).wait_send()
                for m in range(1, nh):
                    x_copy(n, m).wait_send()

        return carry

    lax.fori_loop(0, nc + latest + 1, main, 0)

    def stat_rep(m):
        return pltpu.make_async_remote_copy(
            src_ref=sq, dst_ref=stat_a.at[m - 1], send_sem=sas.at[m - 1], recv_sem=sar.at[m - 1],
            device_id={"rep": lax.rem(r + m, nr)}, device_id_type=MESH,
        )

    def stat_tile(m):
        return pltpu.make_async_remote_copy(
            src_ref=mine, dst_ref=stat_b.at[m - 1], send_sem=sbs.at[m - 1], recv_sem=sbr.at[m - 1],
            device_id={"tile": lax.rem(t + m, nt)}, device_id_type=MESH,
        )

    for m in range(1, nr):
        stat_rep(m).start()
    total = sq[...]

    lax.fori_loop(0, line, drain, nc - 1)
    for m in range(nh):
        core_copy(nc - 1, m).wait_send()
    for m in range(1, nh):
        x_copy(nc - 1, m).wait_send()

    for m in range(1, nr):
        stat_rep(m).wait_recv()
        total = total + stat_a[m - 1]
    mine[...] = total
    for m in range(1, nt):
        stat_tile(m).start()

    def written(j, carry):
        lad_copy(j).wait()
        return carry

    lax.fori_loop(0, nc, written, 0)
    for m in range(1, nr):
        stat_rep(m).wait_send()
    for m in range(1, nt):
        stat_tile(m).wait_recv()
        total = total + stat_b[m - 1]
    mean = jnp.sum(total, keepdims=True) / (rows_all * cols * nt * nr)
    scale = jnp.minimum(1.0, trust / jnp.sqrt(mean + 1e-06))
    scale_out[...] = jnp.broadcast_to(scale, scale_out.shape)
    for m in range(1, nt):
        stat_tile(m).wait_send()


def local(nt, nr, amplitudes, integrals, slot_row, slot_col, slot_count, source, occ_energy, virt_energy):
    rows, cols = amplitudes.shape
    nloc = integrals.shape[1]
    nc = CHUNKS
    rc = rows // nc
    nh = nr // 2
    qr = nt * (cols // BT)
    pairs = PT_DEV * qr
    f32 = jnp.float32
    dma = pltpu.SemaphoreType.DMA
    vmem = pl.BlockSpec(memory_space=pltpu.VMEM)
    anywhere = pl.BlockSpec(memory_space=pl.ANY)
    scratch = [
        pltpu.VMEM((nt, rows, cols), jnp.bfloat16),
        pltpu.VMEM((nloc + 1, BT, BT), jnp.bfloat16),
        pltpu.VMEM((PT_DEV * BT, nt * cols), jnp.bfloat16),
        pltpu.VMEM((8, pairs), jnp.int32),
        pltpu.SMEM((8, pairs), jnp.int32),
        pltpu.VMEM((rows, 1), f32),
        pltpu.VMEM((nc, nh, rc, cols), f32),
        pltpu.VMEM((nc, nh, rc, cols), f32),
        pltpu.VMEM((nc, nh, rc, cols), f32),
        pltpu.VMEM((nc, nh - 1, rc, cols), f32),
        pltpu.VMEM((nc, nh - 1, rc, cols), f32),
        pltpu.VMEM((rows, cols), f32),
        pltpu.VMEM((rows, cols), f32),
        pltpu.VMEM((8, BT), f32),
        pltpu.VMEM((nr - 1, 8, BT), f32),
        pltpu.VMEM((nt - 1, 8, BT), f32),
        pltpu.VMEM((8, BT), f32),
        dma((nt, nc)), dma((nt, nc)), dma((nt, nc)), dma((nt, nc)),
        dma((nc, nh)), dma((nc, nh)), dma((nc, nh - 1)), dma((nc, nh - 1)),
        dma((nr - 1,)), dma((nr - 1,)), dma((nt - 1,)), dma((nt - 1,)),
        dma((4,)), dma((nc,)),
    ]
    ladder, scale = pl.pallas_call(
        functools.partial(kernel, nt, nr, nc),
        out_shape=(jax.ShapeDtypeStruct((rows, cols), f32), jax.ShapeDtypeStruct((1, cols), f32)),
        in_specs=[anywhere, anywhere, vmem, vmem, vmem, anywhere, vmem, vmem],
        out_specs=(anywhere, vmem),
        scratch_shapes=scratch,
        compiler_params=pltpu.CompilerParams(
            collective_id=0, has_side_effects=True, vmem_limit_bytes=60 * 1024 * 1024
        ),
        name="ladder",
    )(
        amplitudes, integrals, slot_row, slot_col, slot_count, source,
        occ_energy.reshape(1, rows), virt_energy.reshape(1, cols),
    )
    residual = source + ladder
    step = residual / (virt_energy[None, :] - occ_energy[:, None])
    return residual, amplitudes.astype(f32) + scale * step


def solution(mesh):
    placed = (
        P(None, ("tile", "rep")),
        P("rep", "tile", None, None),
        P("rep", "tile"),
        P("rep", "tile"),
        P("rep", "tile"),
        P(None, ("tile", "rep")),
        P(),
        P(("tile", "rep")),
    )
    return jax.shard_map(
        functools.partial(local, mesh.shape["tile"], mesh.shape["rep"]),
        mesh=mesh,
        in_specs=placed,
        out_specs=(P(None, ("tile", "rep")), P(None, ("tile", "rep"))),
        check_vma=False,
    )
```
